32 devices in a mesh: groups: 2 (over x), tp: 8 (over z, y), role: 2 (over core).
Axes of the slice: x: 2, y: 2, z: 4, core: 2. Of those that a mesh axis runs over, the one named last changes fastest.
Arguments:
- rows_in: bfloat16 [2, 1024, 8192], P('role', 'groups', 'tp'), parts along dimension 1, may hold values from -6 to 6
- norm_gain: bfloat16 [8192], replicated, may hold values from 0.5 to 4
- q_words: int32 [1024, 8192], P(None, 'tp'), may hold values from -2147483648 to 2147483646
- q_scales: bfloat16 [64, 8192], P(None, 'tp'), may hold values from 0.0011978149 to 0.0047912598
- kv_words: int32 [8, 1024, 256], P('tp'), may hold values from -2147483648 to 2147483646, as said below
- kv_scales: bfloat16 [8, 64, 256], P('tp'), may hold values from 0.0012 to 0.0048, as said below
- o_words: int32 [1024, 8192], P('tp'), may hold values from -2147483648 to 2147483646
- o_scales: bfloat16 [64, 8192], P('tp'), may hold values from 0.0011978149 to 0.0047912598
- kv_pool: bfloat16 [8, 2048, 16, 256], P('tp', 'groups'), parts along dimension 1, may hold values from -120 to 120, as said below
- prompt_pages: int32 [32], P('groups'), parts along dimension 0, may hold values from 1 to 8, 32 in all
- page_slots: int32 [64], P('groups'), parts along dimension 0, may hold values from 0 to 1023, as said below
- block_tables: int32 [992, 16], P('groups'), parts along dimension 0, may hold values from 0 to 1023, as said below
- cache_lens: int32 [992], P('groups'), parts along dimension 0, may hold values from 1 to 256
Outputs:
- layer_out: bfloat16 [2, 1024, 8192], P('role', 'groups', 'tp'), parts along dimension 1
The draws below stay inside these ranges and needn't reach their ends.
There are 2 independent parts, one for each index of `groups`. The reference program is written for one: setup_inputs(seed, part) draws one part's arguments, and reference() takes and returns one part's arrays. A program takes and returns all parts, laid end to end along the dimension named above; an argument that names none is the same for every part. Nothing has to cross between parts.
Inputs may be any that keep to these rules, and one draw needn't show every extreme that they name: `kv_words`: entries t and u are equal whenever t * 8 // 8 equals u * 8 // 8. `kv_scales`: entries t and u are equal whenever t * 8 // 8 equals u * 8 // 8. `kv_pool`: entries t and u are equal whenever t * 8 // 8 equals u * 8 // 8. `page_slots`: distinct pages; entry j receives the j-th page of the prompts taken in order. `block_tables`: no entry is one of page_slots; sequences may share pages.
All inputs are finite; a program needn't handle non-finite values.
Results may differ from the reference program's by a relative error of at most 0.015.
The reference program's roundings to bfloat16 on the way count: a program that leaves them out, or rounds other values in their place, can miss the bound.
Values may be sent and summed in bfloat16 or wider, within the bound.
A program may use at most 192 MiB of HBM per device.

```python
import math
import jax
import jax.numpy as jnp
import numpy as np
from jax import lax

D = 8192
QH = 64
KVH = 8
HD = 128
GROUP = 128
PAGE = 16
PROMPTS = 16
MAXP = 16
ROWS = 512
POOL = 1024
MOSTP = 8
N_TP = 8


def slot_tables(key):
    fresh_count = ROWS // PAGE
    order = jax.random.permutation(jax.random.fold_in(key, 11), POOL).astype(jnp.int32)
    fresh = order[:fresh_count]
    spare = order[fresh_count:]
    picks = jax.random.randint(jax.random.fold_in(key, 12), (ROWS - PROMPTS, MAXP), 0, POOL - fresh_count, dtype=jnp.int32)
    return (fresh, spare[picks])


def draw_page_slots(key, part):
    return slot_tables(key)[0]


def draw_block_tables(key, part):
    return slot_tables(key)[1]


def head_copies(values):
    return jnp.repeat(values, N_TP // KVH, axis=0)


def draw_kv_words(key, part):
    words = jax.random.randint(jax.random.fold_in(key, 21), (KVH, D // 8, 2 * HD), -2147483648, 2147483647, dtype=jnp.int32)
    return head_copies(words)


def draw_kv_scales(key, part):
    logs = jax.random.uniform(jax.random.fold_in(key, 22), (KVH, D // GROUP, 2 * HD), jnp.float32, math.log(0.00121), math.log(0.00476))
    return head_copies(jnp.exp(logs)).astype(jnp.bfloat16)


def draw_kv_pool(key, part):
    values = jnp.clip(jax.random.normal(jax.random.fold_in(key, 23), (KVH, POOL, PAGE, 2 * HD), jnp.float32), -6.0, 6.0)
    return head_copies(values).astype(jnp.bfloat16)


def draw_norm_gain(key, part):
    gains = 1.0 + 0.1 * jnp.clip(jax.random.normal(jax.random.fold_in(key, 24), (D,), jnp.float32), -4.0, 4.0)
    return gains.astype(jnp.bfloat16)


def set_ends(result, rng, least, top_value):
    dims = result.shape
    index_at = [jax.random.randint(jax.random.fold_in(rng, axis), (), 0, dims[axis]) for axis in range(len(dims))]
    result = result.at[tuple(index_at)].set(least)
    longest = dims.index(max(dims))
    index_at[longest] = (index_at[longest] + 1) % dims[longest]
    return result.at[tuple(index_at)].set(top_value)


def steps_of(key, shape, pieces, least, largest):
    level, own = 1.0, jax.random.fold_in(key, 6)
    for position, blocks in pieces:
        heights = jnp.exp(jax.random.uniform(jax.random.fold_in(own, position), (blocks,), jnp.float32, least / len(pieces), largest / len(pieces)))
        level = level * jnp.repeat(heights, shape[position] // blocks).reshape([-1 if axis == position else 1 for axis in range(len(shape))])
    return level


def split_up(number_of, total, bound, lean):
    weights = [(1 << 20) // math.isqrt(standing ** lean) + 1 for standing in range(2, number_of + 1)]
    rest, holding = total - bound - (number_of - 1), [1] * (number_of - 1)
    while rest > 0:
        free = [i for i in range(number_of - 1) if holding[i] < bound]
        mass, remaining = sum([weights[i] for i in free]), rest
        for i in free:
            more = min(bound - holding[i], max(1, remaining * weights[i] // mass), rest)
            holding[i] = holding[i] + more
            rest = rest - more
    return np.array([bound] + holding)


def uneven(stream_key, amount, total, bound, lean):
    if amount == 2:
        one = jax.random.randint(stream_key, (), max(1, total - bound), min(bound, total - 1) + 1)
        return jnp.stack([one, total - one])
    sizes = jnp.asarray(split_up(amount, total, bound, lean), jnp.int32)
    couples = (amount - 1) // 2
    donor, taker = sizes[1:1 + 2 * couples:2], sizes[2:2 + 2 * couples:2]
    margin = jnp.minimum(donor - 1, bound - taker)
    shifted = jax.random.randint(jax.random.fold_in(stream_key, 1), (couples,), 0, 1 << 20) % (margin + 1)
    sizes = sizes.at[1:1 + 2 * couples:2].set(donor - shifted).at[2:2 + 2 * couples:2].set(taker + shifted)
    return sizes[jax.random.permutation(jax.random.fold_in(stream_key, 2), amount)]


def centred(stream_key, extent, scale, reach, pieces=(), kind=jnp.bfloat16):
    array = scale * jax.random.normal(stream_key, extent, jnp.float32)
    if pieces:
        array = array * steps_of(stream_key, extent, pieces, -0.22, 0.18)
    return jnp.clip(array, -reach, reach).astype(kind)


def setup_inputs(seed: int = 0, part: int = 0) -> dict:
    streams_of = jax.random.split(jax.random.key(seed), 14)
    part_splits = jax.random.split(jax.random.fold_in(streams_of[13], part), 14)
    rows_in = centred(part_splits[0], (2, ROWS, D), 1.0, 6.0, ((0, 2), (2, 8)))
    norm_gain = draw_norm_gain(jax.random.fold_in(streams_of[13], 71), part)
    q_words = set_ends(jax.random.randint(streams_of[2], (D // 8, QH * HD), -2147483648, 2147483647), jax.random.fold_in(streams_of[2], 1), -2147483648, 2147483646).astype(jnp.int32)
    q_scales = jnp.clip(jnp.exp(math.log(0.0047912598) - 1.3862944 * jax.random.uniform(streams_of[3], (D // GROUP, QH * HD), jnp.float32) ** steps_of(streams_of[3], (D // GROUP, QH * HD), ((1, 8),), -0.2, 0.2)), 0.0011978149, 0.0047912598).astype(jnp.bfloat16)
    kv_words = draw_kv_words(jax.random.fold_in(streams_of[13], 71), part)
    kv_scales = draw_kv_scales(jax.random.fold_in(streams_of[13], 71), part)
    o_words = set_ends(jax.random.randint(streams_of[6], (QH * HD // 8, D), -2147483648, 2147483647), jax.random.fold_in(streams_of[6], 1), -2147483648, 2147483646).astype(jnp.int32)
    o_scales = jnp.clip(jnp.exp(math.log(0.0047912598) - 1.3862944 * jax.random.uniform(streams_of[7], (QH * HD // GROUP, D), jnp.float32) ** steps_of(streams_of[7], (QH * HD // GROUP, D), ((0, 8),), -0.2, 0.2)), 0.0011978149, 0.0047912598).astype(jnp.bfloat16)
    kv_pool = draw_kv_pool(jax.random.fold_in(jax.random.fold_in(streams_of[13], part), 71), part)
    prompt_pages = uneven(part_splits[9], PROMPTS, ROWS // PAGE, MOSTP, 2).astype(jnp.int32)
    page_slots = draw_page_slots(jax.random.fold_in(jax.random.fold_in(streams_of[13], part), 71), part)
    block_tables = draw_block_tables(jax.random.fold_in(jax.random.fold_in(streams_of[13], part), 71), part)
    cache_lens = set_ends(jax.random.randint(part_splits[12], (ROWS - PROMPTS,), 1, MAXP * PAGE + 1), jax.random.fold_in(part_splits[12], 1), 1, MAXP * PAGE).astype(jnp.int32)
    return dict(rows_in=rows_in, norm_gain=norm_gain, q_words=q_words, q_scales=q_scales, kv_words=kv_words, kv_scales=kv_scales, o_words=o_words, o_scales=o_scales, kv_pool=kv_pool, prompt_pages=prompt_pages, page_slots=page_slots, block_tables=block_tables, cache_lens=cache_lens)


def unpack_words(words, scales):
    shifts = jnp.arange(8, dtype=jnp.int32) * 4
    nibbles = jnp.bitwise_and(jnp.right_shift(words[:, None, :], shifts[None, :, None]), 15) - 8
    values = nibbles.reshape(words.shape[0] * 8, words.shape[1]).astype(jnp.float32)
    group = values.shape[0] // scales.shape[0]
    spread = jnp.repeat(scales.astype(jnp.float32), group, axis=0)
    return (values * spread).astype(jnp.bfloat16)

def rms_normed(rows, gain):
    wide = rows.astype(jnp.float32)
    inverse = lax.rsqrt(lax.optimization_barrier(jnp.mean(wide * wide, axis=-1, keepdims=True)) + 1e-05)
    return (wide * inverse * gain.astype(jnp.float32)).astype(jnp.bfloat16)

def rotate(heads, positions):
    half = heads.shape[-1] // 2
    freq = 500000.0 ** (-jnp.arange(half, dtype=jnp.float32) * 2.0 / heads.shape[-1])
    angle = positions.astype(jnp.float32)[:, None, None] * freq[None, None, :]
    cosine = jnp.cos(angle)
    sine = jnp.sin(angle)
    first = heads[..., :half]
    second = heads[..., half:]
    return jnp.concatenate([first * cosine - second * sine, second * cosine + first * sine], axis=-1)

def layout(prompt_pages, page_slots, block_tables, cache_lens, rows):
    page = rows // page_slots.shape[0]
    count = prompt_pages.shape[0]
    ends = (jnp.cumsum(prompt_pages) * page).astype(jnp.int32)
    starts = (ends - prompt_pages * page).astype(jnp.int32)
    index = jnp.arange(rows, dtype=jnp.int32)
    member = (index[:, None] >= starts[None, :]) & (index[:, None] < ends[None, :])
    doc = lax.optimization_barrier(jnp.sum(jnp.where(member, jnp.arange(count, dtype=jnp.int32)[None, :], 0), axis=1)).astype(jnp.int32)
    prefill_pos = (index - lax.optimization_barrier(jnp.sum(jnp.where(member, starts[None, :], 0), axis=1))).astype(jnp.int32)
    span = block_tables.shape[1]
    picks = jnp.minimum(starts[:, None] // page + jnp.arange(span, dtype=jnp.int32)[None, :], page_slots.shape[0] - 1)
    prompt_table = page_slots[picks.astype(jnp.int32)]
    table = jnp.concatenate([prompt_table, block_tables], axis=0).astype(jnp.int32)
    lengths = jnp.concatenate([prompt_pages * page, cache_lens]).astype(jnp.int32)
    return (doc, prefill_pos, table, lengths)

def prefill_attend(query, keys, values, doc):
    rows = query.shape[0]
    block = min(512, rows)
    score_scale = query.shape[-1] ** (-0.5)
    index = jnp.arange(rows, dtype=jnp.int32)

    def one_block(start):
        partial_query = lax.dynamic_slice_in_dim(query, start, block, 0).astype(jnp.float32)
        logit_scores = jnp.einsum('qhd,kd->hqk', partial_query, keys.astype(jnp.float32)) * score_scale
        own = start + jnp.arange(block, dtype=jnp.int32)
        own_doc = lax.dynamic_slice_in_dim(doc, start, block, 0)
        allowed = (own_doc[:, None] == doc[None, :]) & (index[None, :] <= own[:, None])
        logit_scores = jnp.where(allowed[None], logit_scores, -1e+30)
        attention_probs = jax.nn.softmax(logit_scores, axis=-1).astype(jnp.bfloat16)
        return jnp.einsum('hqk,kd->qhd', attention_probs.astype(jnp.float32), values.astype(jnp.float32)).astype(jnp.bfloat16)
    starts = jnp.arange(0, rows, block, dtype=jnp.int32)
    done = lax.map(one_block, starts)
    return done.reshape(rows, query.shape[1], query.shape[2])

def decode_attend(query, key_self, value_self, cache, table, lengths):
    rows = query.shape[0]
    block = min(128, rows)
    score_scale = query.shape[-1] ** (-0.5)
    head_dim = query.shape[-1]

    def one_block(start):
        partial_query = lax.dynamic_slice_in_dim(query, start, block, 0).astype(jnp.float32)
        part_table = lax.dynamic_slice_in_dim(table, start, block, 0)
        part_len = lax.dynamic_slice_in_dim(lengths, start, block, 0)
        pages = cache[part_table]
        pages = pages.reshape(block, pages.shape[1] * pages.shape[2], pages.shape[3])
        own_key = lax.dynamic_slice_in_dim(key_self, start, block, 0)
        own_value = lax.dynamic_slice_in_dim(value_self, start, block, 0)
        gathered_keys = jnp.concatenate([pages[..., :head_dim], own_key[:, None, :]], axis=1)
        gathered_values = jnp.concatenate([pages[..., head_dim:], own_value[:, None, :]], axis=1)
        logit_scores = jnp.einsum('jai,jri->jar', partial_query, gathered_keys.astype(jnp.float32)) * score_scale
        spots = jnp.arange(pages.shape[1], dtype=jnp.int32)
        valid = jnp.concatenate([spots[None, :] < part_len[:, None], jnp.ones((block, 1), dtype=bool)], axis=1)
        logit_scores = jnp.where(valid[:, None, :], logit_scores, -1e+30)
        attention_probs = jax.nn.softmax(logit_scores, axis=-1).astype(jnp.bfloat16)
        return jnp.einsum('cwt,ctr->cwr', attention_probs.astype(jnp.float32), gathered_values.astype(jnp.float32)).astype(jnp.bfloat16)
    starts = jnp.arange(0, rows, block, dtype=jnp.int32)
    done = lax.map(one_block, starts)
    return done.reshape(rows, query.shape[1], query.shape[2])

def reference(rows_in, norm_gain, q_words, q_scales, kv_words, kv_scales, o_words, o_scales, kv_pool, prompt_pages, page_slots, block_tables, cache_lens):
    copies = N_TP // KVH
    group_heads = QH // KVH
    doc, prefill_pos, table, lengths = layout(prompt_pages, page_slots, block_tables, cache_lens, ROWS)
    w_query = unpack_words(q_words, q_scales)
    w_out = unpack_words(o_words, o_scales)
    normed = [rms_normed(rows_in[0], norm_gain), rms_normed(rows_in[1], norm_gain)]
    positions = [prefill_pos, lengths]
    queries = []
    for side in range(2):
        projected = jnp.dot(normed[side], w_query, preferred_element_type=jnp.float32).reshape(ROWS, QH, HD)
        queries.append(rotate(projected, positions[side]).astype(jnp.bfloat16))
    attention_output = [[], []]
    for head in range(KVH):
        w_keyval = unpack_words(kv_words[head * copies], kv_scales[head * copies])
        keys = []
        values = []
        for side in range(2):
            keyval = jnp.dot(normed[side], w_keyval, preferred_element_type=jnp.float32)
            keys.append(rotate(keyval[:, None, :HD], positions[side])[:, 0].astype(jnp.bfloat16))
            values.append(keyval[:, HD:].astype(jnp.bfloat16))
        fresh = jnp.concatenate([keys[0], values[0]], axis=1).reshape(ROWS // PAGE, PAGE, 2 * HD)
        cache = kv_pool[head * copies].at[page_slots].set(fresh)
        lower = head * group_heads
        attention_output[0].append(prefill_attend(queries[0][:, lower:lower + group_heads], keys[0], values[0], doc))
        attention_output[1].append(decode_attend(queries[1][:, lower:lower + group_heads], keys[1], values[1], cache, table, lengths))
    results = []
    for side in range(2):
        joined = jnp.concatenate(attention_output[side], axis=1).reshape(ROWS, QH * HD)
        results.append(jnp.dot(joined, w_out, preferred_element_type=jnp.float32).astype(jnp.bfloat16))
    return jnp.stack(results)
```

```python
import jax
import jax.numpy as jnp
from jax import lax
from jax.experimental import pallas as pl
from jax.experimental.pallas import tpu as pltpu
from jax.sharding import PartitionSpec as P

HD = 128


def passed_along(block, axis, distance):
    devices = range(lax.axis_size(axis))
    route = [(i - distance, i) for i in devices if i - distance in devices]
    return lax.ppermute(block, axis, route)


def unpack_words(words, scales):
    shifts = jnp.arange(8, dtype=jnp.int32) * 4
    nibbles = jnp.bitwise_and(jnp.right_shift(words[:, None, :], shifts[None, :, None]), 15) - 8
    values = nibbles.reshape(words.shape[0] * 8, words.shape[1]).astype(jnp.float32)
    group = values.shape[0] // scales.shape[0]
    spread = jnp.repeat(scales.astype(jnp.float32), group, axis=0)
    return (values * spread).astype(jnp.bfloat16)


def rms_normed(rows, gain):
    wide = rows.astype(jnp.float32)
    inverse = lax.rsqrt(jnp.mean(wide * wide, axis=-1, keepdims=True) + 1e-05)
    return (wide * inverse * gain.astype(jnp.float32)).astype(jnp.bfloat16)


def rotate(heads, positions):
    half = heads.shape[-1] // 2
    freq = 500000.0 ** (-jnp.arange(half, dtype=jnp.float32) * 2.0 / heads.shape[-1])
    angle = positions.astype(jnp.float32)[:, None, None] * freq[None, None, :]
    cosine = jnp.cos(angle)
    sine = jnp.sin(angle)
    first = heads[..., :half]
    second = heads[..., half:]
    return jnp.concatenate(
        [first * cosine - second * sine, second * cosine + first * sine], axis=-1
    )


def layout(prompt_pages, page_slots, block_tables, cache_lens, rows):
    page = rows // page_slots.shape[0]
    count = prompt_pages.shape[0]
    ends = jnp.cumsum(prompt_pages) * page
    starts = ends - prompt_pages * page
    index = jnp.arange(rows, dtype=jnp.int32)
    member = (index[:, None] >= starts[None, :]) & (index[:, None] < ends[None, :])
    doc = jnp.sum(jnp.where(member, jnp.arange(count, dtype=jnp.int32)[None, :], 0), axis=1)
    prefill_pos = index - jnp.sum(jnp.where(member, starts[None, :], 0), axis=1)
    span = block_tables.shape[1]
    picks = jnp.minimum(
        starts[:, None] // page + jnp.arange(span, dtype=jnp.int32)[None, :],
        page_slots.shape[0] - 1,
    )
    prompt_table = page_slots[picks]
    table = jnp.concatenate([prompt_table, block_tables], axis=0)
    lengths = jnp.concatenate([prompt_pages * page, cache_lens])
    return (doc, prefill_pos, table, lengths)


def prefill_attend(query, keys, values, doc):
    rows = query.shape[0]
    block = min(512, rows)
    score_scale = query.shape[-1] ** (-0.5)
    index = jnp.arange(rows, dtype=jnp.int32)

    def prefill_one_block(start):
        logit_scores = (
            jnp.einsum("qhd,kd->hqk", query, keys, preferred_element_type=jnp.float32) * score_scale
        )
        own = start + jnp.arange(block, dtype=jnp.int32)
        allowed = (doc[:, None] == doc[None, :]) & (index[None, :] <= own[:, None])
        logit_scores = jnp.where(allowed[None], logit_scores, -1e30)
        attention_probs = jax.nn.softmax(logit_scores, axis=-1).astype(jnp.bfloat16)
        return jnp.einsum(
            "hqk,kd->qhd", attention_probs, values, preferred_element_type=jnp.float32
        ).astype(jnp.bfloat16)

    starts = jnp.arange(0, rows, block, dtype=jnp.int32)
    done = lax.map(prefill_one_block, starts)
    return done.reshape(rows, query.shape[1], query.shape[2])


def decode_kernel(table_ref, slots_ref, q_ref, own_ref, len_ref, fresh_ref, pool_ref, out_ref,
                  cache, scores, weights, sem):
    group, heads, head_dim = q_ref.shape
    span = table_ref.shape[1]
    page = cache.shape[1]
    tokens = span * page
    step = pl.program_id(0)

    @pl.when(step == 0)
    def _():
        load = pltpu.make_async_copy(pool_ref, cache, sem)
        load.start()
        load.wait()

        def place(j, carry):
            cache[slots_ref[j]] = fresh_ref[j]
            return carry

        lax.fori_loop(0, slots_ref.shape[0], place, 0)

    def pages(b, low):
        picked = [
            cache[table_ref[step * group + b, p], :, low : low + head_dim] for p in range(span)
        ]
        return jnp.concatenate(picked, axis=0)

    for b in range(group):
        scores[b] = lax.dot_general(
            q_ref[b], pages(b, 0), (((1,), (1,)), ((), ())), preferred_element_type=jnp.float32
        )
    scale = head_dim ** (-0.5)
    spots = lax.broadcasted_iota(jnp.int32, (group, heads, tokens), 2)
    valid = spots < len_ref[...][:, :, :1]
    s = jnp.where(valid, scores[...] * scale, -1e30)
    own_key = own_ref[:, :, :head_dim].astype(jnp.float32)
    own_value = own_ref[:, :, head_dim:].astype(jnp.float32)
    own = jnp.sum(q_ref[...].astype(jnp.float32) * own_key, axis=-1, keepdims=True) * scale
    top = jnp.maximum(jnp.max(s, axis=-1, keepdims=True), own)
    e = jnp.exp(s - top)
    e_own = jnp.exp(own - top)
    inverse = 1.0 / (jnp.sum(e, axis=-1, keepdims=True) + e_own)
    weights[...] = (e * inverse).astype(jnp.bfloat16)
    mine = (e_own * inverse).astype(jnp.bfloat16).astype(jnp.float32) * own_value
    for b in range(group):
        out_ref[b] = (
            jnp.dot(weights[b], pages(b, head_dim), preferred_element_type=jnp.float32) + mine[b]
        ).astype(jnp.bfloat16)


def decode_attend(query, own, fresh, pool, page_slots, table, lengths):
    rows, heads, head_dim = query.shape
    group = 16 if rows % 16 == 0 else 1
    tokens = table.shape[1] * pool.shape[1]
    wide = jnp.broadcast_to(lengths[:, None, None], (rows, 1, 128))
    return pl.pallas_call(
        decode_kernel,
        grid_spec=pltpu.PrefetchScalarGridSpec(
            num_scalar_prefetch=2,
            grid=(rows // group,),
            in_specs=[
                pl.BlockSpec((group, heads, head_dim), lambda g, *_: (g, 0, 0)),
                pl.BlockSpec((group, 1, 2 * head_dim), lambda g, *_: (g, 0, 0)),
                pl.BlockSpec((group, 1, 128), lambda g, *_: (g, 0, 0)),
                pl.BlockSpec(memory_space=pltpu.VMEM),
                pl.BlockSpec(memory_space=pl.ANY),
            ],
            out_specs=pl.BlockSpec((group, heads, head_dim), lambda g, *_: (g, 0, 0)),
            scratch_shapes=[
                pltpu.VMEM(pool.shape, pool.dtype),
                pltpu.VMEM((group, heads, tokens), jnp.float32),
                pltpu.VMEM((group, heads, tokens), jnp.bfloat16),
                pltpu.SemaphoreType.DMA(()),
            ],
        ),
        out_shape=jax.ShapeDtypeStruct(query.shape, jnp.bfloat16),
        compiler_params=pltpu.CompilerParams(vmem_limit_bytes=40 << 20),
    )(table, page_slots, query, own[:, None, :], wide, fresh, pool)


def local(
    rows_in,
    norm_gain,
    q_words,
    q_scales,
    kv_words,
    kv_scales,
    o_words,
    o_scales,
    kv_pool,
    prompt_pages,
    page_slots,
    block_tables,
    cache_lens,
):
    side = lax.axis_index("role")
    whole = lax.all_gather(rows_in[0], "tp", axis=1, tiled=True)
    rows = whole.shape[0]
    normed = rms_normed(whole, norm_gain)
    doc, prefill_pos, table, lengths = layout(
        prompt_pages, page_slots, block_tables, cache_lens, rows
    )
    positions = jnp.where(side == 0, prefill_pos, lengths)
    w_query = unpack_words(q_words, q_scales)
    w_keyval = unpack_words(kv_words[0], kv_scales[0])
    projected = jnp.dot(normed, w_query, preferred_element_type=jnp.float32)
    query = rotate(projected.reshape(rows, -1, HD), positions).astype(jnp.bfloat16)
    keyval = jnp.dot(normed, w_keyval, preferred_element_type=jnp.float32)
    key_new = rotate(keyval[:, None, :HD], positions)[:, 0].astype(jnp.bfloat16)
    value_new = keyval[:, HD:].astype(jnp.bfloat16)
    fresh = jnp.concatenate([key_new, value_new], axis=1)
    arrived = passed_along(fresh, "role", 1)
    pool = kv_pool[0]

    def run_prefill():
        return prefill_attend(query, key_new, value_new, doc)

    def run_decode():
        pages = arrived.reshape(-1, pool.shape[1], pool.shape[2])
        return decode_attend(query, fresh, pages, pool, page_slots, table, lengths)

    attention_output = lax.cond(side == 0, run_prefill, run_decode).reshape(rows, -1)
    w_rows = unpack_words(o_words, o_scales)
    partial = jnp.dot(attention_output, w_rows, preferred_element_type=jnp.float32)
    summed = lax.psum_scatter(
        partial.astype(jnp.bfloat16), "tp", scatter_dimension=1, tiled=True
    )
    return summed[None]


def solution(mesh):
    return jax.shard_map(
        local,
        mesh=mesh,
        in_specs=(
            P("role", "groups", "tp"),
            P(),
            P(None, "tp"),
            P(None, "tp"),
            P("tp", None, None),
            P("tp", None, None),
            P("tp", None),
            P("tp", None),
            P("tp", "groups", None, None),
            P("groups"),
            P("groups"),
            P("groups", None),
            P("groups"),
        ),
        out_specs=P("role", "groups", "tp"),
        check_vma=False,
    )
```

```python
import functools

import jax
import jax.numpy as jnp
from jax import lax
from jax.experimental import pallas as pl
from jax.experimental.pallas import tpu as pltpu
from jax.sharding import PartitionSpec as P

HD = 128


def passed_along(block, axis, distance):
    devices = range(lax.axis_size(axis))
    route = [(i - distance, i) for i in devices if i - distance in devices]
    return lax.ppermute(block, axis, route)


def unpack_words(words, scales):
    shifts = jnp.arange(8, dtype=jnp.int32) * 4
    nibbles = jnp.bitwise_and(jnp.right_shift(words[:, None, :], shifts[None, :, None]), 15) - 8
    values = nibbles.reshape(words.shape[0] * 8, words.shape[1]).astype(jnp.float32)
    group = values.shape[0] // scales.shape[0]
    spread = jnp.repeat(scales.astype(jnp.float32), group, axis=0)
    return (values * spread).astype(jnp.bfloat16)


def rms_normed(rows, gain):
    wide = rows.astype(jnp.float32)
    inverse = lax.rsqrt(jnp.mean(wide * wide, axis=-1, keepdims=True) + 1e-05)
    return (wide * inverse * gain.astype(jnp.float32)).astype(jnp.bfloat16)


def rotate(heads, positions):
    half = heads.shape[-1] // 2
    freq = 500000.0 ** (-jnp.arange(half, dtype=jnp.float32) * 2.0 / heads.shape[-1])
    angle = positions.astype(jnp.float32)[:, None, None] * freq[None, None, :]
    cosine = jnp.cos(angle)
    sine = jnp.sin(angle)
    first = heads[..., :half]
    second = heads[..., half:]
    return jnp.concatenate(
        [first * cosine - second * sine, second * cosine + first * sine], axis=-1
    )


def layout(prompt_pages, page_slots, block_tables, cache_lens, rows):
    page = rows // page_slots.shape[0]
    count = prompt_pages.shape[0]
    ends = jnp.cumsum(prompt_pages) * page
    starts = ends - prompt_pages * page
    index = jnp.arange(rows, dtype=jnp.int32)
    member = (index[:, None] >= starts[None, :]) & (index[:, None] < ends[None, :])
    doc = jnp.sum(jnp.where(member, jnp.arange(count, dtype=jnp.int32)[None, :], 0), axis=1)
    prefill_pos = index - jnp.sum(jnp.where(member, starts[None, :], 0), axis=1)
    span = block_tables.shape[1]
    picks = jnp.minimum(
        starts[:, None] // page + jnp.arange(span, dtype=jnp.int32)[None, :],
        page_slots.shape[0] - 1,
    )
    prompt_table = page_slots[picks]
    table = jnp.concatenate([prompt_table, block_tables], axis=0)
    lengths = jnp.concatenate([prompt_pages * page, cache_lens])
    return (doc, prefill_pos, table, lengths)


def prefill_attend(query, keys, values, doc):
    rows = query.shape[0]
    block = min(512, rows)
    score_scale = query.shape[-1] ** (-0.5)
    index = jnp.arange(rows, dtype=jnp.int32)

    def prefill_one_block(start):
        logit_scores = (
            jnp.einsum("qhd,kd->hqk", query, keys, preferred_element_type=jnp.float32) * score_scale
        )
        own = start + jnp.arange(block, dtype=jnp.int32)
        allowed = (doc[:, None] == doc[None, :]) & (index[None, :] <= own[:, None])
        logit_scores = jnp.where(allowed[None], logit_scores, -1e30)
        attention_probs = jax.nn.softmax(logit_scores, axis=-1).astype(jnp.bfloat16)
        return jnp.einsum(
            "hqk,kd->qhd", attention_probs, values, preferred_element_type=jnp.float32
        ).astype(jnp.bfloat16)

    starts = jnp.arange(0, rows, block, dtype=jnp.int32)
    done = lax.map(prefill_one_block, starts)
    return done.reshape(rows, query.shape[1], query.shape[2])


def decode_kernel(table_ref, slots_ref, q_ref, own_ref, len_ref, fresh_ref, pool_ref, out_ref,
                  cache, scores, weights, sem):
    group, heads, head_dim = q_ref.shape
    span = table_ref.shape[1]
    page = cache.shape[1]
    tokens = span * page
    step = pl.program_id(0)

    @pl.when(step == 0)
    def _():
        load = pltpu.make_async_copy(pool_ref, cache, sem)
        load.start()
        load.wait()

        def place(j, carry):
            cache[slots_ref[j]] = fresh_ref[j]
            return carry

        lax.fori_loop(0, slots_ref.shape[0], place, 0)

    def pages(b, low):
        picked = [
            cache[table_ref[step * group + b, p], :, low : low + head_dim] for p in range(span)
        ]
        return jnp.concatenate(picked, axis=0)

    for b in range(group):
        scores[b] = lax.dot_general(
            q_ref[b], pages(b, 0), (((1,), (1,)), ((), ())), preferred_element_type=jnp.float32
        )
    scale = head_dim ** (-0.5)
    spots = lax.broadcasted_iota(jnp.int32, (group, heads, tokens), 2)
    valid = spots < len_ref[...][:, :, :1]
    s = jnp.where(valid, scores[...] * scale, -1e30)
    own_key = own_ref[:, :, :head_dim].astype(jnp.float32)
    own_value = own_ref[:, :, head_dim:].astype(jnp.float32)
    own = jnp.sum(q_ref[...].astype(jnp.float32) * own_key, axis=-1, keepdims=True) * scale
    top = jnp.maximum(jnp.max(s, axis=-1, keepdims=True), own)
    e = jnp.exp(s - top)
    e_own = jnp.exp(own - top)
    inverse = 1.0 / (jnp.sum(e, axis=-1, keepdims=True) + e_own)
    weights[...] = (e * inverse).astype(jnp.bfloat16)
    mine = (e_own * inverse).astype(jnp.bfloat16).astype(jnp.float32) * own_value
    for b in range(group):
        out_ref[b] = (
            jnp.dot(weights[b], pages(b, head_dim), preferred_element_type=jnp.float32) + mine[b]
        ).astype(jnp.bfloat16)


def decode_attend(query, own, fresh, pool, page_slots, table, lengths):
    rows, heads, head_dim = query.shape
    group = 16 if rows % 16 == 0 else 1
    tokens = table.shape[1] * pool.shape[1]
    wide = jnp.broadcast_to(lengths[:, None, None], (rows, 1, 128))
    return pl.pallas_call(
        decode_kernel,
        grid_spec=pltpu.PrefetchScalarGridSpec(
            num_scalar_prefetch=2,
            grid=(rows // group,),
            in_specs=[
                pl.BlockSpec((group, heads, head_dim), lambda g, *_: (g, 0, 0)),
                pl.BlockSpec((group, 1, 2 * head_dim), lambda g, *_: (g, 0, 0)),
                pl.BlockSpec((group, 1, 128), lambda g, *_: (g, 0, 0)),
                pl.BlockSpec(memory_space=pltpu.VMEM),
                pl.BlockSpec(memory_space=pl.ANY),
            ],
            out_specs=pl.BlockSpec((group, heads, head_dim), lambda g, *_: (g, 0, 0)),
            scratch_shapes=[
                pltpu.VMEM(pool.shape, pool.dtype),
                pltpu.VMEM((group, heads, tokens), jnp.float32),
                pltpu.VMEM((group, heads, tokens), jnp.bfloat16),
                pltpu.SemaphoreType.DMA(()),
            ],
        ),
        out_shape=jax.ShapeDtypeStruct(query.shape, jnp.bfloat16),
        compiler_params=pltpu.CompilerParams(vmem_limit_bytes=40 << 20),
    )(table, page_slots, query, own[:, None, :], wide, fresh, pool)


def project_kernel(n, pair, x_ref, w_ref, out_ref, w_here, y_out, y_in, z_out, up_in, down_in,
                   w_sem, y_sent, y_got, z_sent, up_got, down_got):
    me = lax.axis_index("tp")
    length = n // pair
    z, y = me // pair, me % pair
    width = out_ref.shape[1]
    tile = min(256, width)
    tiles = width // tile

    def greet(device):
        pl.semaphore_signal(
            barrier, inc=1, device_id={"tp": device}, device_id_type=pl.DeviceIdType.MESH
        )

    def load(dest):
        start = pl.multiple_of(dest * width, width)
        return pltpu.make_async_copy(
            w_ref.at[:, pl.ds(start, width)], w_here.at[dest], w_sem.at[dest]
        )

    def send(source, target, sent, got, device):
        return pltpu.make_async_remote_copy(
            src_ref=source,
            dst_ref=target,
            send_sem=sent,
            recv_sem=got,
            device_id={"tp": device},
            device_id_type=pl.DeviceIdType.MESH,
        )

    def across(d):
        return send(y_out.at[d], y_in.at[d], y_sent.at[d], y_got.at[d], z * pair + 1 - y)

    def upward(d):
        return send(z_out.at[d], up_in.at[d], z_sent.at[d], up_got.at[d], me + pair)

    def downward(d):
        return send(z_out.at[d], down_in.at[d], z_sent.at[d], down_got.at[d], me - pair)

    def in_order(above, below):
        def both(j, carry):
            @pl.when(length - 1 - j > z)
            def _():
                above(length - 1 - j)

            @pl.when(j < z)
            def _():
                below(j)

            return carry

        lax.fori_loop(0, length - 1, both, 0)

    def product(dest, put):
        load(dest).wait()

        def one(c, carry):
            columns = pl.ds(pl.multiple_of(c * tile, tile), tile)
            put(
                columns,
                jnp.dot(x_ref[...], w_here[dest, :, columns], preferred_element_type=jnp.float32),
            )
            return carry

        lax.fori_loop(0, tiles, one, 0)

    def swap(d):
        def put(columns, value):
            y_out[d, :, columns] = value.astype(jnp.bfloat16)

        product(d * pair + 1 - y, put)
        across(d).start()

    def total(d, target, extra):
        if pair > 1:
            across(d).wait_recv()

        def put(columns, value):
            if pair > 1:
                value = value + y_in[d, :, columns].astype(jnp.float32)
            for block in extra:
                value = value + block[d, :, columns].astype(jnp.float32)
            target(columns, value.astype(jnp.bfloat16))

        product(d * pair + y, put)

    def chain(d, arriving, got, has, pass_on):
        def store(columns, value):
            z_out[d, :, columns] = value

        @pl.when(has)
        def _():
            got(d).wait_recv()
            total(d, store, (arriving,))

        @pl.when(jnp.logical_not(has))
        def _():
            total(d, store, ())

        pass_on(d).start()

    if pair > 1:
        in_order(
            lambda d: load(d * pair + 1 - y).start(), lambda d: load(d * pair + 1 - y).start()
        )
        load(z * pair + 1 - y).start()
    in_order(lambda d: load(d * pair + y).start(), lambda d: load(d * pair + y).start())
    load(z * pair + y).start()

    barrier = pltpu.get_barrier_semaphore()
    has_lower, has_upper = z > 0, z < length - 1
    if pair > 1:
        greet(z * pair + 1 - y)

    @pl.when(has_lower)
    def _():
        greet(me - pair)

    @pl.when(has_upper)
    def _():
        greet(me + pair)

    lower, upper = (z + length - 1) // length, 1 - (z + 1) // length
    pl.semaphore_wait(barrier, pair - 1 + lower + upper)

    if pair > 1:
        in_order(swap, swap)
        swap(z)
    in_order(
        lambda d: chain(d, up_in, upward, has_lower, upward),
        lambda d: chain(d, down_in, downward, has_upper, downward),
    )

    def finish(columns, value):
        out_ref[:, columns] = value

    @pl.when(has_lower)
    def _():
        upward(z).wait_recv()

    @pl.when(has_upper)
    def _():
        downward(z).wait_recv()

    @pl.when(jnp.logical_and(has_lower, has_upper))
    def _():
        total(z, finish, (up_in, down_in))

    @pl.when(jnp.logical_and(has_lower, jnp.logical_not(has_upper)))
    def _():
        total(z, finish, (up_in,))

    @pl.when(jnp.logical_and(has_upper, jnp.logical_not(has_lower)))
    def _():
        total(z, finish, (down_in,))

    in_order(lambda d: upward(d).wait_send(), lambda d: downward(d).wait_send())
    if pair > 1:
        in_order(lambda d: across(d).wait_send(), lambda d: across(d).wait_send())
        across(z).wait_send()


def project(x, w):
    n = lax.axis_size("tp")
    pair = 2 if n == 8 else 1
    length = n // pair
    rows, depth = x.shape
    width = w.shape[1] // n
    slots = pltpu.VMEM((length, rows, width), jnp.bfloat16)
    crossing = slots if pair > 1 else pltpu.VMEM((1, 16, 128), jnp.bfloat16)
    dma = pltpu.SemaphoreType.DMA((length,))
    return pl.pallas_call(
        functools.partial(project_kernel, n, pair),
        out_shape=jax.ShapeDtypeStruct((rows, width), jnp.bfloat16),
        in_specs=[
            pl.BlockSpec(memory_space=pltpu.VMEM),
            pl.BlockSpec(memory_space=pl.ANY),
        ],
        out_specs=pl.BlockSpec(memory_space=pltpu.VMEM),
        scratch_shapes=[
            pltpu.VMEM((n, depth, width), jnp.bfloat16),
            crossing,
            crossing,
            slots,
            slots,
            slots,
            pltpu.SemaphoreType.DMA((n,)),
            dma,
            dma,
            dma,
            dma,
            dma,
        ],
        compiler_params=pltpu.CompilerParams(
            collective_id=0, has_side_effects=True, vmem_limit_bytes=58 << 20
        ),
    )(x, w)


def local(
    rows_in,
    norm_gain,
    q_words,
    q_scales,
    kv_words,
    kv_scales,
    o_words,
    o_scales,
    kv_pool,
    prompt_pages,
    page_slots,
    block_tables,
    cache_lens,
):
    side = lax.axis_index("role")
    whole = lax.all_gather(rows_in[0], "tp", axis=1, tiled=True)
    rows = whole.shape[0]
    normed = rms_normed(whole, norm_gain)
    doc, prefill_pos, table, lengths = layout(
        prompt_pages, page_slots, block_tables, cache_lens, rows
    )
    positions = jnp.where(side == 0, prefill_pos, lengths)
    w_query = unpack_words(q_words, q_scales)
    w_keyval = unpack_words(kv_words[0], kv_scales[0])
    projected = jnp.dot(normed, w_query, preferred_element_type=jnp.float32)
    query = rotate(projected.reshape(rows, -1, HD), positions).astype(jnp.bfloat16)
    keyval = jnp.dot(normed, w_keyval, preferred_element_type=jnp.float32)
    key_new = rotate(keyval[:, None, :HD], positions)[:, 0].astype(jnp.bfloat16)
    value_new = keyval[:, HD:].astype(jnp.bfloat16)
    fresh = jnp.concatenate([key_new, value_new], axis=1)
    arrived = passed_along(fresh, "role", 1)
    pool = kv_pool[0]

    def run_prefill():
        return prefill_attend(query, key_new, value_new, doc)

    def run_decode():
        pages = arrived.reshape(-1, pool.shape[1], pool.shape[2])
        return decode_attend(query, fresh, pages, pool, page_slots, table, lengths)

    attention_output = lax.cond(side == 0, run_prefill, run_decode).reshape(rows, -1)
    w_rows = unpack_words(o_words, o_scales)
    summed = project(attention_output, w_rows)
    return summed[None]


def solution(mesh):
    return jax.shard_map(
        local,
        mesh=mesh,
        in_specs=(
            P("role", "groups", "tp"),
            P(),
            P(None, "tp"),
            P(None, "tp"),
            P("tp", None, None),
            P("tp", None, None),
            P("tp", None),
            P("tp", None),
            P("tp", "groups", None, None),
            P("groups"),
            P("groups"),
            P("groups", None),
            P("groups"),
        ),
        out_specs=P("role", "groups", "tp"),
        check_vma=False,
    )
```
